128 devices in a mesh: groups: 4 (over x, y), seq: 32 (over z, core).
Axes of the slice: x: 2, y: 2, z: 16, core: 2. Of those that a mesh axis runs over, the one named last changes fastest.
The devices are a block of a 8x8x16 slice.
Arguments:
- prefill_keys: bfloat16 [256, 8192, 128], P(('groups', 'seq')), parts along dimension 0, may hold values from -4 to 4
- prefill_values: bfloat16 [256, 8192, 128], P(('groups', 'seq')), parts along dimension 0, may hold values from -6 to 6
- window_queries: bfloat16 [256, 8, 256, 128], P(('groups', 'seq')), parts along dimension 0, may hold values from -48 to 48
- step_queries: bfloat16 [256, 2, 8, 128], P('groups'), parts along dimension 0, may hold values from -48 to 48
- new_keys: bfloat16 [256, 2, 128], P('groups'), parts along dimension 0, may hold values from -24 to 24
- new_values: bfloat16 [256, 2, 128], P('groups'), parts along dimension 0, may hold values from -6 to 6
- lengths: int32 [32], P('groups'), parts along dimension 0, may hold values from 4096 to 8192
- keep_mask: int32 [32, 64], P('groups'), parts along dimension 0, may hold values from 0 to 1, as said below
Outputs:
- cache_keys: bfloat16 [256, 8192, 128], P('groups', 'seq'), parts along dimension 0
- cache_values: bfloat16 [256, 8192, 128], P('groups', 'seq'), parts along dimension 0
- attended: bfloat16 [256, 2, 8, 128], P('groups'), parts along dimension 0
- block_scores: float32 [256, 64], P('groups', 'seq'), parts along dimension 0
The draws below stay inside these ranges and needn't reach their ends.
There are 4 independent parts, one for each index of `groups`. The reference program is written for one: setup_inputs(seed, part) draws one part's arguments, and reference() takes and returns one part's arrays. A program takes and returns all parts, laid end to end along the dimension named above; each array names one. Nothing has to cross between parts.
Inputs may be any that keep to these rules, and one draw needn't show every extreme that they name: `keep_mask`: 1 keeps a block, 0 drops it; block 0 of every sequence is kept.
All inputs are finite; a program needn't handle non-finite values.
Results may differ from the reference program's by a relative error of at most 0.0055.
Values may be sent and summed in bfloat16 or wider, within the bound.
A program may use at most 128 MiB of HBM per device.

```python
import math
import jax
import jax.numpy as jnp
from jax import lax

KVH = 8
GROUP = 8
HD = 128
SEQS = 8
BLOCK = 128
WIN = 256
STEPS = 2
PAIRS = 64
LEN = 8192
NBLK = 64


def first_keys(key):
    return jnp.clip(jax.random.normal(jax.random.fold_in(key, 12), (PAIRS, HD), jnp.float32), -4.0, 4.0)


def draw_prefill_keys(key, part):
    entries = jnp.clip(jax.random.normal(jax.random.fold_in(key, 11), (PAIRS, LEN, HD), jnp.float32), -4.0, 4.0)
    return entries.at[:, 0, :].set(first_keys(key)).astype(jnp.bfloat16)


def draw_window_queries(key, part):
    sample = 3.0 * jnp.clip(jax.random.normal(jax.random.fold_in(key, 21), (PAIRS, GROUP, WIN, HD), jnp.float32), -4.0, 4.0)
    return sample.astype(jnp.bfloat16)


def plain_steps(key):
    return 3.0 * jnp.clip(jax.random.normal(jax.random.fold_in(key, 31), (PAIRS, STEPS, GROUP, HD), jnp.float32), -4.0, 4.0)


def step_sample(key):
    sample = plain_steps(key)
    return sample


def draw_step_queries(key, part):
    return step_sample(key).astype(jnp.bfloat16)


def draw_new_keys(key, part):
    centre = jnp.mean(plain_steps(key)[:, :, 1:, :].astype(jnp.bfloat16).astype(jnp.float32), axis=2)
    extra = jnp.clip(jax.random.normal(jax.random.fold_in(key, 41), (PAIRS, STEPS, HD), jnp.float32), -4.0, 4.0)
    return (centre + extra).astype(jnp.bfloat16)


def draw_keep_mask(key, part):
    picked = jax.random.randint(jax.random.fold_in(key, 51), (SEQS, NBLK), 0, 4)
    return jnp.where(picked < 3, 1, 0).astype(jnp.int32).at[:, 0].set(1)


def plant(result, stream_key, low, largest):
    longest = result.shape.index(max(result.shape))
    spots = []
    for shift in (0, 1):
        where = [jax.random.randint(jax.random.fold_in(stream_key, axis), (), 0, length) for axis, length in enumerate(result.shape)]
        where[longest] = (where[longest] + shift) % result.shape[longest]
        spots.append(tuple(where))
    return result.at[spots[0]].set(low).at[spots[1]].set(largest)


def level_of(own_key, extent, cuts, smallest, high):
    loudness = 1.0
    for dim, blocks in cuts:
        draws = jax.random.uniform(jax.random.fold_in(jax.random.fold_in(own_key, 6), dim), (blocks,), jnp.float32, smallest / len(cuts), high / len(cuts))
        loudness = loudness * jnp.repeat(jnp.exp(draws), extent[dim] // blocks).reshape((-1,) + (1,) * (len(extent) - 1 - dim))
    return loudness


def noise(key, extent, deviation, reach, shards=(), held_as=jnp.bfloat16):
    factor_of = level_of(key, extent, shards, -0.22, 0.18) if shards else 1.0
    drawn = jax.random.normal(key, extent, jnp.float32) * deviation * factor_of
    return jnp.minimum(jnp.maximum(drawn, -reach), reach).astype(held_as)


def setup_inputs(seed: int = 0, part: int = 0) -> dict:
    splits = jax.random.split(jax.random.key(seed), 9)
    part_splits = jax.random.split(jax.random.fold_in(splits[8], part), 9)
    prefill_keys = draw_prefill_keys(jax.random.fold_in(jax.random.fold_in(splits[8], part), 71), part)
    prefill_values = noise(part_splits[1], (PAIRS, LEN, HD), 1.0, 6.0, ((0, 32),))
    window_queries = draw_window_queries(jax.random.fold_in(jax.random.fold_in(splits[8], part), 71), part)
    step_queries = draw_step_queries(jax.random.fold_in(jax.random.fold_in(splits[8], part), 71), part)
    new_keys = draw_new_keys(jax.random.fold_in(jax.random.fold_in(splits[8], part), 71), part)
    new_values = noise(part_splits[5], (PAIRS, STEPS, HD), 1.0, 6.0)
    lengths = plant(jax.random.randint(part_splits[6], (SEQS,), LEN // 2, LEN + 1), jax.random.fold_in(part_splits[6], 1), LEN // 2, LEN).astype(jnp.int32)
    keep_mask = draw_keep_mask(jax.random.fold_in(jax.random.fold_in(splits[8], part), 71), part)
    return dict(prefill_keys=prefill_keys, prefill_values=prefill_values, window_queries=window_queries, step_queries=step_queries, new_keys=new_keys, new_values=new_values, lengths=lengths, keep_mask=keep_mask)


def window_prior(prefill_keys, window_queries, lengths, keep_mask):
    scaling = 1.0 / math.sqrt(HD)
    kept_tokens = jnp.repeat(keep_mask, BLOCK, axis=1) > 0
    position = jnp.arange(LEN, dtype=jnp.int32)
    offsets = jnp.tile(jnp.arange(WIN, dtype=jnp.int32), GROUP)

    def one_pair(pair_id):
        seq_id = pair_id // KVH
        query_rows = window_queries[pair_id].reshape(GROUP * WIN, HD)
        scores = jnp.dot(query_rows, prefill_keys[pair_id].T, preferred_element_type=jnp.float32) * scaling
        query_pos = lengths[seq_id] - WIN + offsets
        visible = kept_tokens[seq_id][None, :] & (position[None, :] <= query_pos[:, None])
        scores = jnp.where(visible, scores, -jnp.inf)
        highest = lax.optimization_barrier(jnp.max(scores, axis=1, keepdims=True))
        weights = jnp.exp(scores - highest)
        probability = weights / lax.optimization_barrier(jnp.sum(weights, axis=1, keepdims=True))
        return lax.optimization_barrier(jnp.sum(probability, axis=0)).reshape(NBLK, BLOCK).sum(axis=1) / GROUP
    return lax.map(one_pair, jnp.arange(PAIRS, dtype=jnp.int32))

def reference(prefill_keys, prefill_values, window_queries, step_queries, new_keys, new_values, lengths, keep_mask):
    prior_mass = window_prior(prefill_keys, window_queries, lengths, keep_mask).astype(jnp.bfloat16)
    scaling = 1.0 / math.sqrt(HD)
    position = jnp.arange(LEN, dtype=jnp.int32)
    kept_tokens = jnp.repeat(keep_mask, BLOCK, axis=1) > 0
    seq_visible = kept_tokens & (position[None, :] < lengths[:, None])
    pair_seq = jnp.arange(PAIRS, dtype=jnp.int32) // KVH
    visible = seq_visible[pair_seq]
    query_rows = step_queries.astype(jnp.float32).reshape(PAIRS, STEPS * GROUP, HD)
    scores = jnp.einsum('pqd,ptd->pqt', query_rows, prefill_keys.astype(jnp.float32), precision=lax.Precision.HIGHEST) * scaling
    scores = jnp.where(visible[:, None, :], scores, -jnp.inf)
    own_scores = jnp.einsum('pqd,pjd->pqj', query_rows, new_keys.astype(jnp.float32), precision=lax.Precision.HIGHEST) * scaling
    row_step = jnp.arange(STEPS * GROUP, dtype=jnp.int32) // GROUP
    own_visible = jnp.arange(STEPS, dtype=jnp.int32)[None, :] <= row_step[:, None]
    own_scores = jnp.where(own_visible[None], own_scores, -jnp.inf)
    highest = jnp.maximum(lax.optimization_barrier(jnp.max(scores, axis=2)), lax.optimization_barrier(jnp.max(own_scores, axis=2)))
    weights = jnp.exp(scores - highest[:, :, None])
    own_weights = jnp.exp(own_scores - highest[:, :, None])
    total_mass = lax.optimization_barrier(jnp.sum(weights, axis=2)) + lax.optimization_barrier(jnp.sum(own_weights, axis=2))
    rounded = lax.optimization_barrier(weights.astype(jnp.bfloat16)).astype(jnp.float32)
    own_rounded = lax.optimization_barrier(own_weights.astype(jnp.bfloat16)).astype(jnp.float32)
    summed = jnp.einsum('pqt,ptd->pqd', rounded, prefill_values.astype(jnp.float32), precision=lax.Precision.HIGHEST)
    summed = summed + jnp.einsum('pqj,pjd->pqd', own_rounded, new_values.astype(jnp.float32), precision=lax.Precision.HIGHEST)
    attended = (summed / total_mass[:, :, None]).astype(jnp.bfloat16).reshape(PAIRS, STEPS, GROUP, HD)
    new_mass = lax.optimization_barrier(jnp.sum(weights / total_mass[:, :, None], axis=1)).reshape(PAIRS, NBLK, BLOCK).sum(axis=2) / GROUP
    block_scores = prior_mass.astype(jnp.float32) + new_mass
    return (prefill_keys, prefill_values, attended, block_scores)
```

```python
import functools
import math

import jax
import jax.numpy as jnp
from jax import lax
from jax.experimental import pallas as pl
from jax.experimental.pallas import tpu as pltpu
from jax.sharding import PartitionSpec as P

KVH = 8
GROUP = 8
BLOCK = 128
LOG2E = 1.4426950408889634
NEG = -1e30
MESH = pl.DeviceIdType.MESH


def remote(src, dst, send_sem, recv_sem, peer):
    return pltpu.make_async_remote_copy(
        src_ref=src,
        dst_ref=dst,
        send_sem=send_sem,
        recv_sem=recv_sem,
        device_id={"seq": peer},
        device_id_type=MESH,
    )


def main_kernel(
    n,
    k_hbm,
    v_hbm,
    wq_hbm,
    sq_hbm,
    nk_hbm,
    nv_hbm,
    lengths_hbm,
    keep_hbm,
    ck,
    cv,
    att,
    sco,
    kbuf,
    vbuf,
    wq,
    sq,
    nk,
    nv,
    lengths_ref,
    keep_smem,
    keep_vmem,
    logits,
    sbuf,
    mbuf,
    wbuf,
    acc,
    mass,
    column,
    message,
    load_sem,
    own_sem,
    send_sem,
    recv_sem,
    small_send,
    small_recv,
):
    pairs, tokens, width = kbuf.shape
    share = tokens // n
    blocks = tokens // BLOCK
    share_blocks = blocks // n
    window = wq.shape[2]
    rows = sq.shape[1]
    chips = n // 2
    me = lax.axis_index("seq")
    z, c = me // 2, me % 2
    first_pair = me * pairs
    seq_id = first_pair // KVH
    scaling = 1.0 / math.sqrt(width)
    fold = scaling * LOG2E

    barrier = pltpu.get_barrier_semaphore()
    for step in range(1, n):
        pl.semaphore_signal(
            barrier, inc=1, device_id={"seq": lax.rem(me + step, n)}, device_id_type=MESH
        )

    loads = [
        pltpu.make_async_copy(k_hbm, kbuf, load_sem.at[0]),
        pltpu.make_async_copy(sq_hbm.at[pl.ds(first_pair, pairs)], sq, load_sem.at[1]),
        pltpu.make_async_copy(nk_hbm.at[pl.ds(first_pair, pairs)], nk, load_sem.at[2]),
        pltpu.make_async_copy(nv_hbm.at[pl.ds(first_pair, pairs)], nv, load_sem.at[3]),
        pltpu.make_async_copy(lengths_hbm, lengths_ref, load_sem.at[4]),
        pltpu.make_async_copy(keep_hbm, keep_smem, load_sem.at[5]),
        pltpu.make_async_copy(keep_hbm, keep_vmem, load_sem.at[6]),
        pltpu.make_async_copy(v_hbm, vbuf, load_sem.at[7]),
        pltpu.make_async_copy(wq_hbm, wq, load_sem.at[8]),
    ]
    for load in loads:
        load.start()
    mine = pl.ds(first_pair, pairs)
    own = [
        pltpu.make_async_copy(
            src.at[:, pl.ds(pl.multiple_of(me * share, share), share), :], dst.at[mine], own_sem.at[i]
        )
        for i, (src, dst) in enumerate(((k_hbm, ck), (v_hbm, cv)))
    ]
    for copy in own:
        copy.start()

    pl.semaphore_wait(barrier, n - 1)

    def send_share(src, dst, i, first, last):
        def one(turn, carry):
            step = jnp.where(turn % 2 == 0, (turn + 1) // 2, n - (turn + 1) // 2)
            peer = lax.rem(me + step, n)
            remote(
                src.at[:, pl.ds(pl.multiple_of(peer * share, share), share), :],
                dst.at[mine],
                send_sem.at[i],
                recv_sem.at[i],
                peer,
            ).start()
            return carry

        lax.fori_loop(first, last, one, 0)

    send_share(k_hbm, ck, 0, 1, n)

    for load in loads[:8]:
        load.wait()
    length = lengths_ref[seq_id]
    chunk = 8 * BLOCK
    chunks = tokens // chunk
    for i in range(pairs):
        query = sq[i]
        lane = lax.broadcasted_iota(jnp.int32, (1, chunk), 1)

        def score_chunk(j, highest):
            base = pl.multiple_of(j * chunk, chunk)
            s = lax.dot_general(
                query,
                kbuf[i, pl.ds(base, chunk), :],
                (((1,), (1,)), ((), ())),
                preferred_element_type=jnp.float32,
            )
            kept = jnp.concatenate(
                [
                    jnp.full((1, BLOCK), keep_smem[seq_id, j * 8 + u], jnp.int32)
                    for u in range(8)
                ],
                axis=1,
            )
            limit = jnp.where(kept > 0, length, 0)
            s = jnp.where(lane + base < limit, s * scaling, NEG)
            logits[:, pl.ds(base, chunk)] = s
            return jnp.maximum(highest, jnp.max(s, axis=1, keepdims=True))

        highest = lax.fori_loop(0, chunks, score_chunk, jnp.full((rows, 1), NEG, jnp.float32))
        steps = nk.shape[1]
        query_f = query.astype(jnp.float32)
        row_step = lax.broadcasted_iota(jnp.int32, (rows, 1), 0) // GROUP
        own_scores = []
        for j in range(steps):
            key_f = nk[i].astype(jnp.float32)[j : j + 1]
            o = jnp.sum(query_f * key_f, axis=1, keepdims=True) * scaling
            o = jnp.where(row_step >= j, o, NEG)
            own_scores.append(o)
            highest = jnp.maximum(highest, o)
        own_weights = [jnp.exp(o - highest) for o in own_scores]
        extra_total = sum(own_weights)
        extra_sum = sum(
            w.astype(jnp.bfloat16).astype(jnp.float32) * nv[i].astype(jnp.float32)[j : j + 1]
            for j, w in enumerate(own_weights)
        )

        def value_chunk(j, carry):
            total, summed = carry
            base = pl.multiple_of(j * chunk, chunk)
            w = jnp.exp(logits[:, pl.ds(base, chunk)] - highest)
            logits[:, pl.ds(base, chunk)] = w
            total = total + jnp.sum(w, axis=1, keepdims=True)
            summed = summed + jnp.dot(
                w.astype(jnp.bfloat16),
                vbuf[i, pl.ds(base, chunk), :],
                preferred_element_type=jnp.float32,
            )
            return total, summed

        total, summed = lax.fori_loop(0, chunks, value_chunk, (extra_total, extra_sum))
        inverse = 1.0 / total
        result = (summed / total).astype(jnp.bfloat16)
        att[z // 4, z % 4, c, i] = result

        def mass_chunk(j, carry):
            base = pl.multiple_of(j * chunk, chunk)
            w = jnp.sum(logits[:, pl.ds(base, chunk)] * inverse, axis=0, keepdims=True)
            tile = jnp.concatenate([w[:, u * BLOCK : (u + 1) * BLOCK] for u in range(8)], axis=0)
            mass[i, pl.ds(pl.multiple_of(j * 8, 8), 8), :] = tile
            return carry

        lax.fori_loop(0, chunks, mass_chunk, 0)

    half = n // 2
    send_share(v_hbm, cv, 1, half, n)

    def chip(step):
        return lax.rem(z + step + chips, chips) * 2 + c

    slot = att.at[z // 4, z % 4, c]
    far = [
        remote(slot, slot, small_send.at[k], small_recv.at[k], chip(step))
        for k, step in enumerate((4, -4, 8))
    ]
    for copy in far:
        copy.start()

    loads[8].wait()
    eye = lax.broadcasted_iota(jnp.int32, (blocks, blocks), 0) == lax.broadcasted_iota(
        jnp.int32, (blocks, blocks), 1
    )
    keep_row = jnp.broadcast_to(keep_vmem[pl.ds(seq_id, 1), :], (blocks, blocks))
    keep_col = jnp.sum(jnp.where(eye, keep_row, 0), axis=1, keepdims=True) > 0
    limit_row = length - window + lax.broadcasted_iota(jnp.int32, (1, window), 1)
    token = lax.broadcasted_iota(jnp.int32, (BLOCK, BLOCK), 0)

    for i in range(pairs):
        acc[...] = jnp.zeros_like(acc)

        def one_group(g, carry):
            query = wq[i, g]

            def one_chunk(j, inner):
                base = pl.multiple_of(j * chunk, chunk)
                sbuf[...] = lax.dot_general(
                    kbuf[i, pl.ds(base, chunk), :],
                    query,
                    (((1,), (1,)), ((), ())),
                    preferred_element_type=jnp.float32,
                )
                here = pl.ds(pl.multiple_of(j * 8, 8), 8)
                for h in range(0, window, BLOCK):
                    tops, sums = [], []
                    for u in range(8):
                        s = sbuf[u * BLOCK : (u + 1) * BLOCK, h : h + BLOCK]
                        s = jnp.where(token <= limit_row[:, h : h + BLOCK] - (base + u * BLOCK), s, NEG)
                        m = jnp.max(s, axis=0, keepdims=True)
                        e = jnp.exp2((s - m) * fold)
                        tops.append(m)
                        sums.append(jnp.sum(e, axis=0, keepdims=True))
                    mbuf[here, h : h + BLOCK] = jnp.concatenate(tops, axis=0)
                    wbuf[here, h : h + BLOCK] = jnp.concatenate(sums, axis=0)
                return inner

            lax.fori_loop(0, chunks, one_chunk, 0)
            m = jnp.where(keep_col, mbuf[...], NEG)
            top = jnp.max(m, axis=0, keepdims=True)
            w = wbuf[...] * jnp.exp2((m - top) * fold)
            acc[...] += w / jnp.sum(w, axis=0, keepdims=True)
            return carry

        lax.fori_loop(0, wq.shape[1], one_group, 0)
        prior = jnp.sum(acc[...], axis=1, keepdims=True) / GROUP
        prior = prior.astype(jnp.bfloat16).astype(jnp.float32)
        new_mass = jnp.sum(mass[i], axis=1, keepdims=True) / GROUP
        column[i] = jnp.broadcast_to(prior + new_mass, (blocks, BLOCK))

    target = lax.broadcasted_iota(jnp.int32, (n, blocks), 0)
    source = lax.broadcasted_iota(jnp.int32, (n, blocks), 1)
    lanes = lax.broadcasted_iota(jnp.int32, (n, BLOCK), 1)
    table = jnp.zeros((n, BLOCK), jnp.float32)
    for i in range(pairs):
        value = column[i][:, :blocks]
        as_row = jnp.sum(jnp.where(eye, value, 0.0), axis=0, keepdims=True)
        for j in range(share_blocks):
            picked = jnp.where(source == target * share_blocks + j, as_row, 0.0)
            entry = jnp.sum(picked, axis=1, keepdims=True)
            table = jnp.where(lanes == i * share_blocks + j, entry, table)
    for d in range(n):
        message[d] = table[d : d + 1]

    for copy in far:
        copy.wait()
    line = att.at[:, z % 4, c]
    near = []
    for k, step in enumerate((1, -1, 2 - 4 * c)):
        near.append(remote(line, line, small_send.at[3 + k], small_recv.at[3 + k], chip(step)))
    for copy in near:
        copy.start()

    def send_scores(step, carry):
        peer = lax.rem(me + step, n)
        remote(message.at[peer], sco.at[me], small_send.at[7], small_recv.at[7], peer).start()
        return carry

    lax.fori_loop(1, n, send_scores, 0)
    keep_own = pltpu.make_async_copy(message.at[me], sco.at[me], own_sem.at[2])
    keep_own.start()

    send_share(v_hbm, cv, 1, 1, half)

    for copy in near:
        copy.wait()
    side = att.at[:, :, c]
    across = remote(side, side, small_send.at[6], small_recv.at[6], me + 1 - 2 * c)
    across.start()

    for copy in own:
        copy.wait()
    keep_own.wait()
    across.wait()
    others = pl.ds(0, (n - 1) * pairs)
    for i, dst in enumerate((ck, cv)):
        pltpu.make_async_copy(dst.at[others], dst.at[others], send_sem.at[i]).wait()
        pltpu.make_async_copy(dst.at[others], dst.at[others], recv_sem.at[i]).wait()
    peers = pl.ds(0, n - 1)
    pltpu.make_async_copy(sco.at[peers], sco.at[peers], small_send.at[7]).wait()
    pltpu.make_async_copy(sco.at[peers], sco.at[peers], small_recv.at[7]).wait()


def write_kernel(ck, cv, att, sco, ck_out, cv_out, att_out, bs_out, sems):
    copies = [
        pltpu.make_async_copy(src, dst, sems.at[i])
        for i, (src, dst) in enumerate(((ck, ck_out), (cv, cv_out), (att, att_out)))
    ]
    for copy in copies:
        copy.start()
    n = sco.shape[0]
    columns, rows = bs_out.shape
    pairs = rows // n
    table = jnp.concatenate([sco[s] for s in range(n)], axis=0)
    source = lax.broadcasted_iota(jnp.int32, (n, rows), 0)
    pair = lax.broadcasted_iota(jnp.int32, (n, rows), 1)
    for j in range(columns):
        total = jnp.zeros((1, rows), jnp.float32)
        for i in range(pairs):
            entry = table[:, i * columns + j : i * columns + j + 1]
            picked = jnp.where(pair == source * pairs + i, entry, 0.0)
            total = total + jnp.sum(picked, axis=0, keepdims=True)
        bs_out[j : j + 1, :] = total
    for copy in copies:
        copy.wait()


def local(
    n,
    prefill_keys,
    prefill_values,
    window_queries,
    step_queries,
    new_keys,
    new_values,
    lengths,
    keep_mask,
):
    pairs, tokens, width = prefill_keys.shape
    all_pairs, steps, group, _ = step_queries.shape
    share = tokens // n
    blocks = tokens // BLOCK
    rows = steps * group
    window = window_queries.shape[2]
    bf16, f32 = jnp.bfloat16, jnp.float32
    anywhere = pl.BlockSpec(memory_space=pl.ANY)
    att_shape = (4, n // 8, 2, pairs, rows, width)
    landed = pl.pallas_call(
        functools.partial(main_kernel, n),
        out_shape=[
            pltpu.VMEM((all_pairs, share, width), bf16),
            pltpu.VMEM((all_pairs, share, width), bf16),
            pltpu.VMEM(att_shape, bf16),
            pltpu.VMEM((n, 1, BLOCK), f32),
        ],
        in_specs=[anywhere] * 8,
        out_specs=[pl.BlockSpec(memory_space=pltpu.VMEM)] * 4,
        scratch_shapes=[
            pltpu.VMEM((pairs, tokens, width), bf16),
            pltpu.VMEM((pairs, tokens, width), bf16),
            pltpu.VMEM(window_queries.shape, bf16),
            pltpu.VMEM((pairs, rows, width), bf16),
            pltpu.VMEM((pairs, steps, width), bf16),
            pltpu.VMEM((pairs, steps, width), bf16),
            pltpu.SMEM(lengths.shape, jnp.int32),
            pltpu.SMEM(keep_mask.shape, jnp.int32),
            pltpu.VMEM(keep_mask.shape, jnp.int32),
            pltpu.VMEM((rows, tokens), f32),
            pltpu.VMEM((8 * BLOCK, window), f32),
            pltpu.VMEM((blocks, window), f32),
            pltpu.VMEM((blocks, window), f32),
            pltpu.VMEM((blocks, window), f32),
            pltpu.VMEM((pairs, blocks, BLOCK), f32),
            pltpu.VMEM((pairs, blocks, BLOCK), f32),
            pltpu.VMEM((n, 1, BLOCK), f32),
            pltpu.SemaphoreType.DMA((9,)),
            pltpu.SemaphoreType.DMA((3,)),
            pltpu.SemaphoreType.DMA((2,)),
            pltpu.SemaphoreType.DMA((2,)),
            pltpu.SemaphoreType.DMA((8,)),
            pltpu.SemaphoreType.DMA((8,)),
        ],
        compiler_params=pltpu.CompilerParams(
            collective_id=0, has_side_effects=True, vmem_limit_bytes=36 * 1024 * 1024
        ),
        name="exchange",
    )(
        *(
            pltpu.with_memory_space_constraint(x, pltpu.HBM)
            for x in (
                prefill_keys,
                prefill_values,
                window_queries,
                step_queries.reshape(all_pairs, rows, width),
                new_keys,
                new_values,
                lengths,
                keep_mask,
            )
        )
    )
    cache_keys, cache_values, attended, block_scores = pl.pallas_call(
        write_kernel,
        out_shape=[
            jax.ShapeDtypeStruct((all_pairs, share, width), bf16),
            jax.ShapeDtypeStruct((all_pairs, share, width), bf16),
            jax.ShapeDtypeStruct(att_shape, bf16),
            jax.ShapeDtypeStruct((blocks // n, all_pairs), f32),
        ],
        in_specs=[anywhere, anywhere, anywhere, pl.BlockSpec(memory_space=pltpu.VMEM)],
        out_specs=[anywhere, anywhere, anywhere, pl.BlockSpec(memory_space=pltpu.VMEM)],
        scratch_shapes=[pltpu.SemaphoreType.DMA((3,))],
        compiler_params=pltpu.CompilerParams(vmem_limit_bytes=4 * 1024 * 1024),
        name="write",
    )(*landed)
    return (
        cache_keys,
        cache_values,
        attended.reshape(all_pairs, steps, group, width),
        block_scores.T,
    )


def solution(mesh):
    placed = (
        P(("groups", "seq"), None, None),
        P(("groups", "seq"), None, None),
        P(("groups", "seq"), None, None, None),
        P("groups", None, None, None),
        P("groups", None, None),
        P("groups", None, None),
        P("groups"),
        P("groups", None),
    )
    return jax.shard_map(
        functools.partial(local, mesh.shape["seq"]),
        mesh=mesh,
        in_specs=placed,
        out_specs=(
            P("groups", "seq", None),
            P("groups", "seq", None),
            P("groups", None, None, None),
            P("groups", "seq"),
        ),
        check_vma=False,
    )
```

```python
import functools
import math

import jax
import jax.numpy as jnp
from jax import lax
from jax.experimental import pallas as pl
from jax.experimental.pallas import tpu as pltpu
from jax.sharding import PartitionSpec as P

KVH = 8
GROUP = 8
BLOCK = 128
LOG2E = 1.4426950408889634
NEG = -1e30
MESH = pl.DeviceIdType.MESH


def remote(src, dst, send_sem, recv_sem, peer):
    return pltpu.make_async_remote_copy(
        src_ref=src,
        dst_ref=dst,
        send_sem=send_sem,
        recv_sem=recv_sem,
        device_id={"seq": peer},
        device_id_type=MESH,
    )


def main_kernel(
    n,
    k_hbm,
    v_hbm,
    wq_hbm,
    sq_hbm,
    nk_hbm,
    nv_hbm,
    lengths_hbm,
    keep_hbm,
    ck,
    cv,
    att,
    sco,
    kbuf,
    vbuf,
    wq,
    sq,
    nk,
    nv,
    lengths_ref,
    keep_smem,
    keep_vmem,
    logits,
    sbuf,
    mbuf,
    wbuf,
    acc,
    mass,
    column,
    message,
    load_sem,
    own_sem,
    send_sem,
    recv_sem,
    small_send,
    small_recv,
):
    pairs, tokens, width = kbuf.shape
    share = tokens // n
    blocks = tokens // BLOCK
    share_blocks = blocks // n
    window = wq.shape[2]
    rows = sq.shape[1]
    chips = n // 2
    me = lax.axis_index("seq")
    z, c = me // 2, me % 2
    first_pair = me * pairs
    seq_id = first_pair // KVH
    scaling = 1.0 / math.sqrt(width)
    fold = scaling * LOG2E

    barrier = pltpu.get_barrier_semaphore()
    for step in range(1, n):
        pl.semaphore_signal(
            barrier, inc=1, device_id={"seq": lax.rem(me + step, n)}, device_id_type=MESH
        )

    loads = [
        pltpu.make_async_copy(k_hbm, kbuf, load_sem.at[0]),
        pltpu.make_async_copy(sq_hbm.at[pl.ds(first_pair, pairs)], sq, load_sem.at[1]),
        pltpu.make_async_copy(nk_hbm.at[pl.ds(first_pair, pairs)], nk, load_sem.at[2]),
        pltpu.make_async_copy(nv_hbm.at[pl.ds(first_pair, pairs)], nv, load_sem.at[3]),
        pltpu.make_async_copy(lengths_hbm, lengths_ref, load_sem.at[4]),
        pltpu.make_async_copy(keep_hbm, keep_smem, load_sem.at[5]),
        pltpu.make_async_copy(keep_hbm, keep_vmem, load_sem.at[6]),
        pltpu.make_async_copy(v_hbm, vbuf, load_sem.at[7]),
        pltpu.make_async_copy(wq_hbm, wq, load_sem.at[8]),
    ]
    for load in loads:
        load.start()
    mine = pl.ds(first_pair, pairs)
    own = [
        pltpu.make_async_copy(
            src.at[:, pl.ds(pl.multiple_of(me * share, share), share), :], dst.at[mine], own_sem.at[i]
        )
        for i, (src, dst) in enumerate(((k_hbm, ck), (v_hbm, cv)))
    ]
    for copy in own:
        copy.start()

    pl.semaphore_wait(barrier, n - 1)

    half = n // 2

    def send_share(src, dst, i, first, last):
        def one(turn, carry):
            step = jnp.where(turn % 2 == 0, (turn + 1) // 2, n - (turn + 1) // 2)
            peer = lax.rem(me + step, n)
            remote(
                src.at[:, pl.ds(pl.multiple_of(peer * share, share), share), :],
                dst.at[mine],
                send_sem.at[i],
                recv_sem.at[i],
                peer,
            ).start()
            return carry

        lax.fori_loop(first, last, one, 0)

    send_share(k_hbm, ck, 0, 1, half)
    send_share(v_hbm, cv, 1, 1, half)

    for load in loads[:8]:
        load.wait()
    length = lengths_ref[seq_id]
    chunk = 8 * BLOCK
    chunks = tokens // chunk
    for i in range(pairs):
        query = sq[i]
        lane = lax.broadcasted_iota(jnp.int32, (1, chunk), 1)

        def score_chunk(j, highest):
            base = pl.multiple_of(j * chunk, chunk)
            s = lax.dot_general(
                query,
                kbuf[i, pl.ds(base, chunk), :],
                (((1,), (1,)), ((), ())),
                preferred_element_type=jnp.float32,
            )
            kept = jnp.concatenate(
                [
                    jnp.full((1, BLOCK), keep_smem[seq_id, j * 8 + u], jnp.int32)
                    for u in range(8)
                ],
                axis=1,
            )
            limit = jnp.where(kept > 0, length, 0)
            s = jnp.where(lane + base < limit, s * scaling, NEG)
            logits[:, pl.ds(base, chunk)] = s
            return jnp.maximum(highest, jnp.max(s, axis=1, keepdims=True))

        highest = lax.fori_loop(0, chunks, score_chunk, jnp.full((rows, 1), NEG, jnp.float32))
        steps = nk.shape[1]
        query_f = query.astype(jnp.float32)
        row_step = lax.broadcasted_iota(jnp.int32, (rows, 1), 0) // GROUP
        own_scores = []
        for j in range(steps):
            key_f = nk[i].astype(jnp.float32)[j : j + 1]
            o = jnp.sum(query_f * key_f, axis=1, keepdims=True) * scaling
            o = jnp.where(row_step >= j, o, NEG)
            own_scores.append(o)
            highest = jnp.maximum(highest, o)
        own_weights = [jnp.exp(o - highest) for o in own_scores]
        extra_total = sum(own_weights)
        extra_sum = sum(
            w.astype(jnp.bfloat16).astype(jnp.float32) * nv[i].astype(jnp.float32)[j : j + 1]
            for j, w in enumerate(own_weights)
        )

        def value_chunk(j, carry):
            total, summed = carry
            base = pl.multiple_of(j * chunk, chunk)
            w = jnp.exp(logits[:, pl.ds(base, chunk)] - highest)
            logits[:, pl.ds(base, chunk)] = w
            total = total + jnp.sum(w, axis=1, keepdims=True)
            summed = summed + jnp.dot(
                w.astype(jnp.bfloat16),
                vbuf[i, pl.ds(base, chunk), :],
                preferred_element_type=jnp.float32,
            )
            return total, summed

        total, summed = lax.fori_loop(0, chunks, value_chunk, (extra_total, extra_sum))
        inverse = 1.0 / total
        result = (summed / total).astype(jnp.bfloat16)
        att[z // 4, z % 4, c, i] = result

        def mass_chunk(j, carry):
            base = pl.multiple_of(j * chunk, chunk)
            w = jnp.sum(logits[:, pl.ds(base, chunk)] * inverse, axis=0, keepdims=True)
            tile = jnp.concatenate([w[:, u * BLOCK : (u + 1) * BLOCK] for u in range(8)], axis=0)
            mass[i, pl.ds(pl.multiple_of(j * 8, 8), 8), :] = tile
            return carry

        lax.fori_loop(0, chunks, mass_chunk, 0)


    def chip(step):
        return lax.rem(z + step + chips, chips) * 2 + c

    slot = att.at[z // 4, z % 4, c]
    far = [
        remote(slot, slot, small_send.at[k], small_recv.at[k], chip(step))
        for k, step in enumerate((4, -4, 8))
    ]
    for copy in far:
        copy.start()

    send_share(k_hbm, ck, 0, half, n)
    loads[8].wait()
    eye = lax.broadcasted_iota(jnp.int32, (blocks, blocks), 0) == lax.broadcasted_iota(
        jnp.int32, (blocks, blocks), 1
    )
    keep_row = jnp.broadcast_to(keep_vmem[pl.ds(seq_id, 1), :], (blocks, blocks))
    keep_col = jnp.sum(jnp.where(eye, keep_row, 0), axis=1, keepdims=True) > 0
    limit_row = length - window + lax.broadcasted_iota(jnp.int32, (1, window), 1)
    token = lax.broadcasted_iota(jnp.int32, (BLOCK, BLOCK), 0)

    for i in range(pairs):
        acc[...] = jnp.zeros_like(acc)

        def one_group(g, carry):
            query = wq[i, g]

            def one_chunk(j, inner):
                base = pl.multiple_of(j * chunk, chunk)
                sbuf[...] = lax.dot_general(
                    kbuf[i, pl.ds(base, chunk), :],
                    query,
                    (((1,), (1,)), ((), ())),
                    preferred_element_type=jnp.float32,
                )
                here = pl.ds(pl.multiple_of(j * 8, 8), 8)
                for h in range(0, window, BLOCK):
                    tops, sums = [], []
                    for u in range(8):
                        s = sbuf[u * BLOCK : (u + 1) * BLOCK, h : h + BLOCK]
                        s = jnp.where(token <= limit_row[:, h : h + BLOCK] - (base + u * BLOCK), s, NEG)
                        m = jnp.max(s, axis=0, keepdims=True)
                        e = jnp.exp2((s - m) * fold)
                        tops.append(m)
                        sums.append(jnp.sum(e, axis=0, keepdims=True))
                    mbuf[here, h : h + BLOCK] = jnp.concatenate(tops, axis=0)
                    wbuf[here, h : h + BLOCK] = jnp.concatenate(sums, axis=0)
                return inner

            lax.fori_loop(0, chunks, one_chunk, 0)
            m = jnp.where(keep_col, mbuf[...], NEG)
            top = jnp.max(m, axis=0, keepdims=True)
            w = wbuf[...] * jnp.exp2((m - top) * fold)
            acc[...] += w / jnp.sum(w, axis=0, keepdims=True)
            return carry

        lax.fori_loop(0, wq.shape[1], one_group, 0)
        prior = jnp.sum(acc[...], axis=1, keepdims=True) / GROUP
        prior = prior.astype(jnp.bfloat16).astype(jnp.float32)
        new_mass = jnp.sum(mass[i], axis=1, keepdims=True) / GROUP
        column[i] = jnp.broadcast_to(prior + new_mass, (blocks, BLOCK))

    target = lax.broadcasted_iota(jnp.int32, (n, blocks), 0)
    source = lax.broadcasted_iota(jnp.int32, (n, blocks), 1)
    lanes = lax.broadcasted_iota(jnp.int32, (n, BLOCK), 1)
    table = jnp.zeros((n, BLOCK), jnp.float32)
    for i in range(pairs):
        value = column[i][:, :blocks]
        as_row = jnp.sum(jnp.where(eye, value, 0.0), axis=0, keepdims=True)
        for j in range(share_blocks):
            picked = jnp.where(source == target * share_blocks + j, as_row, 0.0)
            entry = jnp.sum(picked, axis=1, keepdims=True)
            table = jnp.where(lanes == i * share_blocks + j, entry, table)
    for d in range(n):
        message[d] = table[d : d + 1]

    for copy in far:
        copy.wait()
    line = att.at[:, z % 4, c]
    near = []
    for k, step in enumerate((1, -1, 2 - 4 * c)):
        near.append(remote(line, line, small_send.at[3 + k], small_recv.at[3 + k], chip(step)))
    for copy in near:
        copy.start()

    def send_scores(step, carry):
        peer = lax.rem(me + step, n)
        remote(message.at[peer], sco.at[me], small_send.at[7], small_recv.at[7], peer).start()
        return carry

    lax.fori_loop(1, n, send_scores, 0)
    keep_own = pltpu.make_async_copy(message.at[me], sco.at[me], own_sem.at[2])
    keep_own.start()

    send_share(v_hbm, cv, 1, half, n)

    for copy in near:
        copy.wait()
    side = att.at[:, :, c]
    across = remote(side, side, small_send.at[6], small_recv.at[6], me + 1 - 2 * c)
    across.start()

    for copy in own:
        copy.wait()
    keep_own.wait()
    across.wait()
    others = pl.ds(0, (n - 1) * pairs)
    for i, dst in enumerate((ck, cv)):
        pltpu.make_async_copy(dst.at[others], dst.at[others], send_sem.at[i]).wait()
        pltpu.make_async_copy(dst.at[others], dst.at[others], recv_sem.at[i]).wait()
    peers = pl.ds(0, n - 1)
    pltpu.make_async_copy(sco.at[peers], sco.at[peers], small_send.at[7]).wait()
    pltpu.make_async_copy(sco.at[peers], sco.at[peers], small_recv.at[7]).wait()


def write_kernel(ck, cv, att, sco, ck_out, cv_out, att_out, bs_out, sems):
    copies = [
        pltpu.make_async_copy(src, dst, sems.at[i])
        for i, (src, dst) in enumerate(((ck, ck_out), (cv, cv_out), (att, att_out)))
    ]
    for copy in copies:
        copy.start()
    n = sco.shape[0]
    columns, rows = bs_out.shape
    pairs = rows // n
    table = jnp.concatenate([sco[s] for s in range(n)], axis=0)
    source = lax.broadcasted_iota(jnp.int32, (n, rows), 0)
    pair = lax.broadcasted_iota(jnp.int32, (n, rows), 1)
    for j in range(columns):
        total = jnp.zeros((1, rows), jnp.float32)
        for i in range(pairs):
            entry = table[:, i * columns + j : i * columns + j + 1]
            picked = jnp.where(pair == source * pairs + i, entry, 0.0)
            total = total + jnp.sum(picked, axis=0, keepdims=True)
        bs_out[j : j + 1, :] = total
    for copy in copies:
        copy.wait()


def local(
    n,
    prefill_keys,
    prefill_values,
    window_queries,
    step_queries,
    new_keys,
    new_values,
    lengths,
    keep_mask,
):
    pairs, tokens, width = prefill_keys.shape
    all_pairs, steps, group, _ = step_queries.shape
    share = tokens // n
    blocks = tokens // BLOCK
    rows = steps * group
    window = window_queries.shape[2]
    bf16, f32 = jnp.bfloat16, jnp.float32
    anywhere = pl.BlockSpec(memory_space=pl.ANY)
    att_shape = (4, n // 8, 2, pairs, rows, width)
    landed = pl.pallas_call(
        functools.partial(main_kernel, n),
        out_shape=[
            pltpu.VMEM((all_pairs, share, width), bf16),
            pltpu.VMEM((all_pairs, share, width), bf16),
            pltpu.VMEM(att_shape, bf16),
            pltpu.VMEM((n, 1, BLOCK), f32),
        ],
        in_specs=[anywhere] * 8,
        out_specs=[pl.BlockSpec(memory_space=pltpu.VMEM)] * 4,
        scratch_shapes=[
            pltpu.VMEM((pairs, tokens, width), bf16),
            pltpu.VMEM((pairs, tokens, width), bf16),
            pltpu.VMEM(window_queries.shape, bf16),
            pltpu.VMEM((pairs, rows, width), bf16),
            pltpu.VMEM((pairs, steps, width), bf16),
            pltpu.VMEM((pairs, steps, width), bf16),
            pltpu.SMEM(lengths.shape, jnp.int32),
            pltpu.SMEM(keep_mask.shape, jnp.int32),
            pltpu.VMEM(keep_mask.shape, jnp.int32),
            pltpu.VMEM((rows, tokens), f32),
            pltpu.VMEM((8 * BLOCK, window), f32),
            pltpu.VMEM((blocks, window), f32),
            pltpu.VMEM((blocks, window), f32),
            pltpu.VMEM((blocks, window), f32),
            pltpu.VMEM((pairs, blocks, BLOCK), f32),
            pltpu.VMEM((pairs, blocks, BLOCK), f32),
            pltpu.VMEM((n, 1, BLOCK), f32),
            pltpu.SemaphoreType.DMA((9,)),
            pltpu.SemaphoreType.DMA((3,)),
            pltpu.SemaphoreType.DMA((2,)),
            pltpu.SemaphoreType.DMA((2,)),
            pltpu.SemaphoreType.DMA((8,)),
            pltpu.SemaphoreType.DMA((8,)),
        ],
        compiler_params=pltpu.CompilerParams(
            collective_id=0, has_side_effects=True, vmem_limit_bytes=36 * 1024 * 1024
        ),
        name="exchange",
    )(
        *(
            pltpu.with_memory_space_constraint(x, pltpu.HBM)
            for x in (
                prefill_keys,
                prefill_values,
                window_queries,
                step_queries.reshape(all_pairs, rows, width),
                new_keys,
                new_values,
                lengths,
                keep_mask,
            )
        )
    )
    cache_keys, cache_values, attended, block_scores = pl.pallas_call(
        write_kernel,
        out_shape=[
            jax.ShapeDtypeStruct((all_pairs, share, width), bf16),
            jax.ShapeDtypeStruct((all_pairs, share, width), bf16),
            jax.ShapeDtypeStruct(att_shape, bf16),
            jax.ShapeDtypeStruct((blocks // n, all_pairs), f32),
        ],
        in_specs=[anywhere, anywhere, anywhere, pl.BlockSpec(memory_space=pltpu.VMEM)],
        out_specs=[anywhere, anywhere, anywhere, pl.BlockSpec(memory_space=pltpu.VMEM)],
        scratch_shapes=[pltpu.SemaphoreType.DMA((3,))],
        compiler_params=pltpu.CompilerParams(vmem_limit_bytes=4 * 1024 * 1024),
        name="write",
    )(*landed)
    return (
        cache_keys,
        cache_values,
        attended.reshape(all_pairs, steps, group, width),
        block_scores.T,
    )


def solution(mesh):
    placed = (
        P(("groups", "seq"), None, None),
        P(("groups", "seq"), None, None),
        P(("groups", "seq"), None, None, None),
        P("groups", None, None, None),
        P("groups", None, None),
        P("groups", None, None),
        P("groups"),
        P("groups", None),
    )
    return jax.shard_map(
        functools.partial(local, mesh.shape["seq"]),
        mesh=mesh,
        in_specs=placed,
        out_specs=(
            P("groups", "seq", None),
            P("groups", "seq", None),
            P("groups", None, None, None),
            P("groups", "seq"),
        ),
        check_vma=False,
    )
```

```python
import functools
import math

import jax
import jax.numpy as jnp
from jax import lax
from jax.experimental import pallas as pl
from jax.experimental.pallas import tpu as pltpu
from jax.sharding import PartitionSpec as P

KVH = 8
GROUP = 8
BLOCK = 128
LOG2E = 1.4426950408889634
NEG = -1e30
MESH = pl.DeviceIdType.MESH


def remote(src, dst, send_sem, recv_sem, peer):
    return pltpu.make_async_remote_copy(
        src_ref=src,
        dst_ref=dst,
        send_sem=send_sem,
        recv_sem=recv_sem,
        device_id={"seq": peer},
        device_id_type=MESH,
    )


def main_kernel(
    n,
    k_hbm,
    v_hbm,
    wq_hbm,
    sq_hbm,
    nk_hbm,
    nv_hbm,
    lengths_hbm,
    keep_hbm,
    ck,
    cv,
    att,
    sco,
    kbuf,
    vbuf,
    wq,
    sq,
    nk,
    nv,
    lengths_ref,
    keep_smem,
    keep_vmem,
    logits,
    sbuf,
    mbuf,
    wbuf,
    acc,
    mass,
    column,
    message,
    load_sem,
    own_sem,
    send_sem,
    recv_sem,
    small_send,
    small_recv,
    met_sem,
):
    pairs, tokens, width = kbuf.shape
    share = tokens // n
    blocks = tokens // BLOCK
    share_blocks = blocks // n
    window = wq.shape[2]
    rows = sq.shape[1]
    chips = n // 2
    me = lax.axis_index("seq")
    z, c = me // 2, me % 2
    first_pair = me * pairs
    seq_id = first_pair // KVH
    scaling = 1.0 / math.sqrt(width)
    fold = scaling * LOG2E

    barrier = pltpu.get_barrier_semaphore()
    reach = n // 4
    for step in range(reach, 0, -1):
        for peer in (lax.rem(me + step, n), lax.rem(me + n - step, n)):
            pl.semaphore_signal(barrier, inc=1, device_id={"seq": peer}, device_id_type=MESH)

    loads = [
        pltpu.make_async_copy(k_hbm, kbuf, load_sem.at[0]),
        pltpu.make_async_copy(sq_hbm.at[pl.ds(first_pair, pairs)], sq, load_sem.at[1]),
        pltpu.make_async_copy(nk_hbm.at[pl.ds(first_pair, pairs)], nk, load_sem.at[2]),
        pltpu.make_async_copy(nv_hbm.at[pl.ds(first_pair, pairs)], nv, load_sem.at[3]),
        pltpu.make_async_copy(lengths_hbm, lengths_ref, load_sem.at[4]),
        pltpu.make_async_copy(keep_hbm, keep_smem, load_sem.at[5]),
        pltpu.make_async_copy(keep_hbm, keep_vmem, load_sem.at[6]),
        pltpu.make_async_copy(v_hbm, vbuf, load_sem.at[7]),
        pltpu.make_async_copy(wq_hbm, wq, load_sem.at[8]),
    ]
    for load in loads:
        load.start()
    mine = pl.ds(first_pair, pairs)
    own = [
        pltpu.make_async_copy(
            src.at[:, pl.ds(pl.multiple_of(me * share, share), share), :], dst.at[mine], own_sem.at[i]
        )
        for i, (src, dst) in enumerate(((k_hbm, ck), (v_hbm, cv)))
    ]
    for copy in own:
        copy.start()

    pl.semaphore_wait(barrier, 2 * reach)
    for peer in (lax.rem(me + reach, n), lax.rem(me + n - reach, n)):
        pl.semaphore_signal(met_sem, inc=1, device_id={"seq": peer}, device_id_type=MESH)

    half = n // 2

    def send_share(src, dst, i, first, last):
        def one(turn, carry):
            step = jnp.where(turn % 2 == 0, (turn + 1) // 2, n - (turn + 1) // 2)
            peer = lax.rem(me + step, n)
            remote(
                src.at[:, pl.ds(pl.multiple_of(peer * share, share), share), :],
                dst.at[mine],
                send_sem.at[i],
                recv_sem.at[i],
                peer,
            ).start()
            return carry

        lax.fori_loop(first, last, one, 0)

    send_share(k_hbm, ck, 0, 1, half)
    send_share(v_hbm, cv, 1, 1, half)

    for load in loads[:8]:
        load.wait()
    length = lengths_ref[seq_id]
    chunk = 8 * BLOCK
    chunks = tokens // chunk
    for i in range(pairs):
        query = sq[i]
        lane = lax.broadcasted_iota(jnp.int32, (1, chunk), 1)

        def score_chunk(j, highest):
            base = pl.multiple_of(j * chunk, chunk)
            s = lax.dot_general(
                query,
                kbuf[i, pl.ds(base, chunk), :],
                (((1,), (1,)), ((), ())),
                preferred_element_type=jnp.float32,
            )
            kept = jnp.concatenate(
                [
                    jnp.full((1, BLOCK), keep_smem[seq_id, j * 8 + u], jnp.int32)
                    for u in range(8)
                ],
                axis=1,
            )
            limit = jnp.where(kept > 0, length, 0)
            s = jnp.where(lane + base < limit, s * scaling, NEG)
            logits[:, pl.ds(base, chunk)] = s
            return jnp.maximum(highest, jnp.max(s, axis=1, keepdims=True))

        highest = lax.fori_loop(0, chunks, score_chunk, jnp.full((rows, 1), NEG, jnp.float32))
        steps = nk.shape[1]
        query_f = query.astype(jnp.float32)
        row_step = lax.broadcasted_iota(jnp.int32, (rows, 1), 0) // GROUP
        own_scores = []
        for j in range(steps):
            key_f = nk[i].astype(jnp.float32)[j : j + 1]
            o = jnp.sum(query_f * key_f, axis=1, keepdims=True) * scaling
            o = jnp.where(row_step >= j, o, NEG)
            own_scores.append(o)
            highest = jnp.maximum(highest, o)
        own_weights = [jnp.exp(o - highest) for o in own_scores]
        extra_total = sum(own_weights)
        extra_sum = sum(
            w.astype(jnp.bfloat16).astype(jnp.float32) * nv[i].astype(jnp.float32)[j : j + 1]
            for j, w in enumerate(own_weights)
        )

        def value_chunk(j, carry):
            total, summed = carry
            base = pl.multiple_of(j * chunk, chunk)
            w = jnp.exp(logits[:, pl.ds(base, chunk)] - highest)
            logits[:, pl.ds(base, chunk)] = w
            total = total + jnp.sum(w, axis=1, keepdims=True)
            summed = summed + jnp.dot(
                w.astype(jnp.bfloat16),
                vbuf[i, pl.ds(base, chunk), :],
                preferred_element_type=jnp.float32,
            )
            return total, summed

        total, summed = lax.fori_loop(0, chunks, value_chunk, (extra_total, extra_sum))
        inverse = 1.0 / total
        result = (summed / total).astype(jnp.bfloat16)
        att[z // 4, z % 4, c, i] = result

        def mass_chunk(j, carry):
            base = pl.multiple_of(j * chunk, chunk)
            w = jnp.sum(logits[:, pl.ds(base, chunk)] * inverse, axis=0, keepdims=True)
            tile = jnp.concatenate([w[:, u * BLOCK : (u + 1) * BLOCK] for u in range(8)], axis=0)
            mass[i, pl.ds(pl.multiple_of(j * 8, 8), 8), :] = tile
            return carry

        lax.fori_loop(0, chunks, mass_chunk, 0)


    pl.semaphore_wait(met_sem, 2)

    def chip(step):
        return lax.rem(z + step + chips, chips) * 2 + c

    slot = att.at[z // 4, z % 4, c]
    far = [
        remote(slot, slot, small_send.at[k], small_recv.at[k], chip(step))
        for k, step in enumerate((4, -4, 8))
    ]
    for copy in far:
        copy.start()

    send_share(k_hbm, ck, 0, half, n)
    loads[8].wait()
    eye = lax.broadcasted_iota(jnp.int32, (blocks, blocks), 0) == lax.broadcasted_iota(
        jnp.int32, (blocks, blocks), 1
    )
    keep_row = jnp.broadcast_to(keep_vmem[pl.ds(seq_id, 1), :], (blocks, blocks))
    keep_col = jnp.sum(jnp.where(eye, keep_row, 0), axis=1, keepdims=True) > 0
    limit_row = length - window + lax.broadcasted_iota(jnp.int32, (1, window), 1)
    token = lax.broadcasted_iota(jnp.int32, (BLOCK, BLOCK), 0)

    for i in range(pairs):
        acc[...] = jnp.zeros_like(acc)

        def one_group(g, carry):
            query = wq[i, g]

            def one_chunk(j, inner):
                base = pl.multiple_of(j * chunk, chunk)
                sbuf[...] = lax.dot_general(
                    kbuf[i, pl.ds(base, chunk), :],
                    query,
                    (((1,), (1,)), ((), ())),
                    preferred_element_type=jnp.float32,
                )
                here = pl.ds(pl.multiple_of(j * 8, 8), 8)
                for h in range(0, window, BLOCK):
                    tops, sums = [], []
                    for u in range(8):
                        s = sbuf[u * BLOCK : (u + 1) * BLOCK, h : h + BLOCK]
                        s = jnp.where(token <= limit_row[:, h : h + BLOCK] - (base + u * BLOCK), s, NEG)
                        m = jnp.max(s, axis=0, keepdims=True)
                        e = jnp.exp2((s - m) * fold)
                        tops.append(m)
                        sums.append(jnp.sum(e, axis=0, keepdims=True))
                    mbuf[here, h : h + BLOCK] = jnp.concatenate(tops, axis=0)
                    wbuf[here, h : h + BLOCK] = jnp.concatenate(sums, axis=0)
                return inner

            lax.fori_loop(0, chunks, one_chunk, 0)
            m = jnp.where(keep_col, mbuf[...], NEG)
            top = jnp.max(m, axis=0, keepdims=True)
            w = wbuf[...] * jnp.exp2((m - top) * fold)
            acc[...] += w / jnp.sum(w, axis=0, keepdims=True)
            return carry

        lax.fori_loop(0, wq.shape[1], one_group, 0)
        prior = jnp.sum(acc[...], axis=1, keepdims=True) / GROUP
        prior = prior.astype(jnp.bfloat16).astype(jnp.float32)
        new_mass = jnp.sum(mass[i], axis=1, keepdims=True) / GROUP
        column[i] = jnp.broadcast_to(prior + new_mass, (blocks, BLOCK))

    target = lax.broadcasted_iota(jnp.int32, (n, blocks), 0)
    source = lax.broadcasted_iota(jnp.int32, (n, blocks), 1)
    lanes = lax.broadcasted_iota(jnp.int32, (n, BLOCK), 1)
    table = jnp.zeros((n, BLOCK), jnp.float32)
    for i in range(pairs):
        value = column[i][:, :blocks]
        as_row = jnp.sum(jnp.where(eye, value, 0.0), axis=0, keepdims=True)
        for j in range(share_blocks):
            picked = jnp.where(source == target * share_blocks + j, as_row, 0.0)
            entry = jnp.sum(picked, axis=1, keepdims=True)
            table = jnp.where(lanes == i * share_blocks + j, entry, table)
    for d in range(n):
        message[d] = table[d : d + 1]

    for copy in far:
        copy.wait()
    line = att.at[:, z % 4, c]
    near = []
    for k, step in enumerate((1, -1, 2 - 4 * c)):
        near.append(remote(line, line, small_send.at[3 + k], small_recv.at[3 + k], chip(step)))
    for copy in near:
        copy.start()

    def send_scores(step, carry):
        peer = lax.rem(me + step, n)
        remote(message.at[peer], sco.at[me], small_send.at[7], small_recv.at[7], peer).start()
        return carry

    lax.fori_loop(1, n, send_scores, 0)
    keep_own = pltpu.make_async_copy(message.at[me], sco.at[me], own_sem.at[2])
    keep_own.start()

    send_share(v_hbm, cv, 1, half, n)

    for copy in near:
        copy.wait()
    side = att.at[:, :, c]
    across = remote(side, side, small_send.at[6], small_recv.at[6], me + 1 - 2 * c)
    across.start()

    for copy in own:
        copy.wait()
    keep_own.wait()
    across.wait()
    others = pl.ds(0, (n - 1) * pairs)
    for i, dst in enumerate((ck, cv)):
        pltpu.make_async_copy(dst.at[others], dst.at[others], send_sem.at[i]).wait()
        pltpu.make_async_copy(dst.at[others], dst.at[others], recv_sem.at[i]).wait()
    peers = pl.ds(0, n - 1)
    pltpu.make_async_copy(sco.at[peers], sco.at[peers], small_send.at[7]).wait()
    pltpu.make_async_copy(sco.at[peers], sco.at[peers], small_recv.at[7]).wait()


def write_kernel(ck, cv, att, sco, ck_out, cv_out, att_out, bs_out, sems):
    copies = [
        pltpu.make_async_copy(src, dst, sems.at[i])
        for i, (src, dst) in enumerate(((ck, ck_out), (cv, cv_out), (att, att_out)))
    ]
    for copy in copies:
        copy.start()
    n = sco.shape[0]
    columns, rows = bs_out.shape
    pairs = rows // n
    table = jnp.concatenate([sco[s] for s in range(n)], axis=0)
    source = lax.broadcasted_iota(jnp.int32, (n, rows), 0)
    pair = lax.broadcasted_iota(jnp.int32, (n, rows), 1)
    for j in range(columns):
        total = jnp.zeros((1, rows), jnp.float32)
        for i in range(pairs):
            entry = table[:, i * columns + j : i * columns + j + 1]
            picked = jnp.where(pair == source * pairs + i, entry, 0.0)
            total = total + jnp.sum(picked, axis=0, keepdims=True)
        bs_out[j : j + 1, :] = total
    for copy in copies:
        copy.wait()


def local(
    n,
    prefill_keys,
    prefill_values,
    window_queries,
    step_queries,
    new_keys,
    new_values,
    lengths,
    keep_mask,
):
    pairs, tokens, width = prefill_keys.shape
    all_pairs, steps, group, _ = step_queries.shape
    share = tokens // n
    blocks = tokens // BLOCK
    rows = steps * group
    window = window_queries.shape[2]
    bf16, f32 = jnp.bfloat16, jnp.float32
    anywhere = pl.BlockSpec(memory_space=pl.ANY)
    att_shape = (4, n // 8, 2, pairs, rows, width)
    landed = pl.pallas_call(
        functools.partial(main_kernel, n),
        out_shape=[
            pltpu.VMEM((all_pairs, share, width), bf16),
            pltpu.VMEM((all_pairs, share, width), bf16),
            pltpu.VMEM(att_shape, bf16),
            pltpu.VMEM((n, 1, BLOCK), f32),
        ],
        in_specs=[anywhere] * 8,
        out_specs=[pl.BlockSpec(memory_space=pltpu.VMEM)] * 4,
        scratch_shapes=[
            pltpu.VMEM((pairs, tokens, width), bf16),
            pltpu.VMEM((pairs, tokens, width), bf16),
            pltpu.VMEM(window_queries.shape, bf16),
            pltpu.VMEM((pairs, rows, width), bf16),
            pltpu.VMEM((pairs, steps, width), bf16),
            pltpu.VMEM((pairs, steps, width), bf16),
            pltpu.SMEM(lengths.shape, jnp.int32),
            pltpu.SMEM(keep_mask.shape, jnp.int32),
            pltpu.VMEM(keep_mask.shape, jnp.int32),
            pltpu.VMEM((rows, tokens), f32),
            pltpu.VMEM((8 * BLOCK, window), f32),
            pltpu.VMEM((blocks, window), f32),
            pltpu.VMEM((blocks, window), f32),
            pltpu.VMEM((blocks, window), f32),
            pltpu.VMEM((pairs, blocks, BLOCK), f32),
            pltpu.VMEM((pairs, blocks, BLOCK), f32),
            pltpu.VMEM((n, 1, BLOCK), f32),
            pltpu.SemaphoreType.DMA((9,)),
            pltpu.SemaphoreType.DMA((3,)),
            pltpu.SemaphoreType.DMA((2,)),
            pltpu.SemaphoreType.DMA((2,)),
            pltpu.SemaphoreType.DMA((8,)),
            pltpu.SemaphoreType.DMA((8,)),
            pltpu.SemaphoreType.REGULAR,
        ],
        compiler_params=pltpu.CompilerParams(
            collective_id=0, has_side_effects=True, vmem_limit_bytes=36 * 1024 * 1024
        ),
        name="exchange",
    )(
        *(
            pltpu.with_memory_space_constraint(x, pltpu.HBM)
            for x in (
                prefill_keys,
                prefill_values,
                window_queries,
                step_queries.reshape(all_pairs, rows, width),
                new_keys,
                new_values,
                lengths,
                keep_mask,
            )
        )
    )
    cache_keys, cache_values, attended, block_scores = pl.pallas_call(
        write_kernel,
        out_shape=[
            jax.ShapeDtypeStruct((all_pairs, share, width), bf16),
            jax.ShapeDtypeStruct((all_pairs, share, width), bf16),
            jax.ShapeDtypeStruct(att_shape, bf16),
            jax.ShapeDtypeStruct((blocks // n, all_pairs), f32),
        ],
        in_specs=[anywhere, anywhere, anywhere, pl.BlockSpec(memory_space=pltpu.VMEM)],
        out_specs=[anywhere, anywhere, anywhere, pl.BlockSpec(memory_space=pltpu.VMEM)],
        scratch_shapes=[pltpu.SemaphoreType.DMA((3,))],
        compiler_params=pltpu.CompilerParams(vmem_limit_bytes=4 * 1024 * 1024),
        name="write",
    )(*landed)
    return (
        cache_keys,
        cache_values,
        attended.reshape(all_pairs, steps, group, width),
        block_scores.T,
    )


def solution(mesh):
    placed = (
        P(("groups", "seq"), None, None),
        P(("groups", "seq"), None, None),
        P(("groups", "seq"), None, None, None),
        P("groups", None, None, None),
        P("groups", None, None),
        P("groups", None, None),
        P("groups"),
        P("groups", None),
    )
    return jax.shard_map(
        functools.partial(local, mesh.shape["seq"]),
        mesh=mesh,
        in_specs=placed,
        out_specs=(
            P("groups", "seq", None),
            P("groups", "seq", None),
            P("groups", None, None, None),
            P("groups", "seq"),
        ),
        check_vma=False,
    )
```
